32 devices in a mesh: grp: 1, tm: 8 (over y, x, core), op: 4 (over z).
Axes of the slice: x: 2, y: 2, z: 4, core: 2. Of those that a mesh axis runs over, the one named last changes fastest.
Arguments:
- sources: bfloat16 [8, 16, 2, 384, 384], P(('grp', 'tm'), 'op'), may hold values from -6 to 6
- sink: bfloat16 [8, 2, 384, 384], P(('grp', 'tm')), may hold values from -0.3125 to 0.3125
- phase: float32 [8, 384], replicated, may hold values from -3.140625 to 3.140625
- task_table: int32 [3, 8, 16], P(None, ('grp', 'tm'), 'op'), may hold values from -1 to 15, as said below
Outputs:
- task_values: float32 [8, 16, 2, 384], P(('grp', 'tm'), 'op')
The draws below stay inside these ranges and needn't reach their ends.
Inputs may be any that keep to these rules, and one draw needn't show every extreme that they name: `task_table`: field 0 lies in 0 to 15, field 1 in 0 to 7, field 2 is -1 (dead slot) or a rank 0 to 1. At each time slice, for every owner s exactly 2 homes have slot s live, and their places are 0 to 1, each once. At each time slice one home has all 4 slots live.
All inputs are finite; a program needn't handle non-finite values.
Results may differ from the reference program's by a relative error of at most 0.004.
Values may be sent and summed in bfloat16 or wider, within the bound.
No kernel may reach another device: no remote copies, remote signals or barrier semaphores. Data moves between devices by JAX's collectives and lax.ppermute only.
A program may use at most 64 MiB of HBM per device.

```python
import jax
import jax.numpy as jnp
from jax import lax

DIM = 384
OPS_DEV = 4
MOMENTA = 8
CAPACITY = 2
TIMES = 8
OPERATORS = 16
TASKS_DEV = 4


def draw_task_table(key, part):
    homes = TASKS_DEV
    slots = TASKS_DEV
    picks = jax.random.randint(jax.random.fold_in(key, 11), (TIMES, homes * slots), 0, 4 * OPS_DEV)
    moments = jax.random.randint(jax.random.fold_in(key, 12), (TIMES, homes * slots), 0, MOMENTA)
    fullest = jax.random.randint(jax.random.fold_in(key, 13), (TIMES,), 0, homes)
    scores = jax.random.randint(jax.random.fold_in(key, 14), (TIMES, slots, homes), 0, 1048576)
    home_ids = jnp.arange(homes, dtype=jnp.int32)
    scores = jnp.where(home_ids[None, None, :] == fullest[:, None, None], -1, scores)
    keyed = scores * homes + home_ids[None, None, :]
    order = jnp.argsort(keyed, axis=-1)
    ranks = jnp.argsort(order, axis=-1)
    places = jnp.where(ranks < CAPACITY, ranks, -1)
    places = jnp.transpose(places, (0, 2, 1)).reshape(TIMES, homes * slots)
    return jnp.stack([picks, moments, places]).astype(jnp.int32)


def shard_levels(own_key, extent, pieces, least, top_value):
    def one(position, shards_of):
        steps = jax.random.uniform(jax.random.fold_in(jax.random.fold_in(own_key, 6), position), (shards_of,), jnp.float32, least / len(pieces), top_value / len(pieces))
        return jnp.repeat(jnp.exp(steps), extent[position] // shards_of).reshape((-1,) + (1,) * (len(extent) - position - 1))

    gain = one(*pieces[0])
    for cut in pieces[1:]:
        gain = gain * one(*cut)
    return gain


def noise(own_key, shape, scale, bound, pieces=(), kind=jnp.bfloat16):
    result = scale * jax.random.normal(own_key, shape, jnp.float32)
    if pieces:
        result = result * shard_levels(own_key, shape, pieces, -0.22, 0.18)
    return jnp.clip(result, -bound, bound).astype(kind)


def setup_inputs(seed: int = 0, part: int = 0) -> dict:
    splits = jax.random.split(jax.random.key(seed), 5)
    part_splits = jax.random.split(jax.random.fold_in(splits[4], part), 5)
    return {
        "sources": noise(part_splits[0], (TIMES, OPERATORS, 2, DIM, DIM), 1.0, 6.0, ((0, 8), (1, 4))),
        "sink": noise(part_splits[1], (TIMES, 2, DIM, DIM), DIM ** -0.5, 0.3125, ((0, 8),)),
        "phase": jnp.clip(jax.random.uniform(splits[2], (MOMENTA, DIM), jnp.float32, -3.140625, 3.140625), -3.140625, 3.140625),
        "task_table": draw_task_table(jax.random.fold_in(jax.random.fold_in(splits[4], part), 71), part),
    }


SEPARATIONS = (-2, -1, 1, 2)


def task_value(source, angle, sink_slice):
    highest = lax.Precision.HIGHEST
    sink_wide = sink_slice.astype(jnp.float32)
    blocks = jnp.einsum("xij,yjl->xyil", source.astype(jnp.float32), sink_wide, precision=highest)
    quark_real = blocks[0, 0] - blocks[1, 1]
    quark_imag = blocks[0, 1] + blocks[1, 0]
    cosine = jnp.cos(angle)[None, :]
    sine = jnp.sin(angle)[None, :]
    phased = jnp.stack([quark_real * cosine - quark_imag * sine, quark_real * sine + quark_imag * cosine])
    phased = phased.astype(jnp.bfloat16).astype(jnp.float32)
    second = jnp.einsum("xil,yjl->xyij", phased, sink_wide, precision=highest)
    loop_real = second[0, 0] + second[1, 1]
    loop_imag = second[1, 0] - second[0, 1]
    diag_real = jnp.sum(loop_real * loop_real.T - loop_imag * loop_imag.T, axis=1)
    diag_imag = jnp.sum(loop_real * loop_imag.T + loop_imag * loop_real.T, axis=1)
    return jnp.stack([diag_real, diag_imag]) / loop_real.shape[0]


def reference(sources, sink, phase, task_table):
    slots = task_table.shape[2]
    offsets = jnp.array(SEPARATIONS, dtype=jnp.int32)

    def one_task(index):
        time_index = index // slots
        slot = index % slots
        pick = task_table[0, time_index, slot]
        moment = task_table[1, time_index, slot]
        place = task_table[2, time_index, slot]
        home = slot // TASKS_DEV
        source_time = (time_index + offsets[pick // OPS_DEV] + TIMES) % TIMES
        operator = home * OPS_DEV + pick % OPS_DEV
        value = task_value(sources[source_time, operator], phase[moment], sink[time_index])
        return value * (place >= 0).astype(jnp.float32)

    values = lax.map(one_task, jnp.arange(TIMES * slots, dtype=jnp.int32))
    return values.reshape(TIMES, slots, 2, values.shape[-1])
```

```python
import functools

import jax
import jax.numpy as jnp
from jax import lax
from jax.experimental import pallas as pl
from jax.experimental.pallas import tpu as pltpu
from jax.sharding import PartitionSpec as P

SEPARATIONS = (-2, -1, 1, 2)


def contract_kernel(items, where_ref, table_ref, sources_ref, cosine_ref, sine_ref, *refs):
    sink_refs, out_ref, block_ref = refs[:items], refs[items], refs[items + 1]
    ops, _, dim, _ = sources_ref.shape
    slots = out_ref.shape[1]
    out_ref[...] = jnp.zeros_like(out_ref)

    for item in range(items):
        start = where_ref[2 * item] * (3 * slots)
        number = where_ref[2 * item + 1]

        def wanted(slot):
            pick = table_ref[start + slot]
            live = table_ref[start + 2 * slots + slot] >= 0
            return jnp.logical_and(live, pick // ops == number)

        some = functools.reduce(jnp.logical_or, [wanted(slot) for slot in range(slots)])

        @pl.when(some)
        def _():
            sink = sink_refs[item]
            block_ref[:dim, :dim] = sink[0]
            block_ref[:dim, dim:] = sink[1]
            block_ref[dim:, :dim] = -sink[1]
            block_ref[dim:, dim:] = sink[0]

            def one(slot, carry):
                @pl.when(wanted(slot))
                def _():
                    op = table_ref[start + slot] % ops
                    moment = table_ref[start + slots + slot]
                    source = jnp.concatenate([sources_ref[op, 0], sources_ref[op, 1]], axis=1)
                    quark = jnp.dot(source, block_ref[...], preferred_element_type=jnp.float32)
                    quark_real, quark_imag = quark[:, :dim], quark[:, dim:]
                    cosine, sine = cosine_ref[moment], sine_ref[moment]
                    phased = jnp.concatenate(
                        [
                            (quark_real * cosine - quark_imag * sine).astype(jnp.bfloat16),
                            (quark_real * sine + quark_imag * cosine).astype(jnp.bfloat16),
                        ],
                        axis=1,
                    )
                    loop = lax.dot_general(
                        phased, block_ref[...], (((1,), (1,)), ((), ())), preferred_element_type=jnp.float32
                    )
                    loop_real, loop_imag = loop[:, :dim], loop[:, dim:]
                    real_t, imag_t = loop_real.T, loop_imag.T
                    scale = 1.0 / dim
                    out_ref[item, slot, 0:1] = scale * jnp.sum(
                        loop_real * real_t - loop_imag * imag_t, axis=0, keepdims=True
                    )
                    out_ref[item, slot, 1:2] = scale * jnp.sum(
                        loop_real * imag_t + loop_imag * real_t, axis=0, keepdims=True
                    )

                return carry

            lax.fori_loop(0, slots, one, 0)


def contract(where, table, sources, cosine, sine, sinks):
    items = len(sinks)
    dim = sources.shape[-1]
    slots = table.shape[-1]
    vmem = pl.BlockSpec(memory_space=pltpu.VMEM)
    smem = pl.BlockSpec(memory_space=pltpu.SMEM)
    return pl.pallas_call(
        functools.partial(contract_kernel, items),
        out_shape=jax.ShapeDtypeStruct((items, slots, 2, dim), jnp.float32),
        in_specs=[smem, smem] + [vmem] * (3 + items),
        out_specs=vmem,
        scratch_shapes=[pltpu.VMEM((2 * dim, 2 * dim), jnp.bfloat16)],
        name=f"contract_{items}",
    )(where, table.reshape(-1), sources, cosine, sine, *sinks)


def shift(values, by):
    length = lax.axis_size("tm")
    return lax.ppermute(values, "tm", [(i, (i + by) % length) for i in range(length)])


def direct(run, sink):
    me = lax.axis_index("tm")
    length = lax.axis_size("tm")
    total = None
    for number, separation in enumerate(SEPARATIONS):
        where = jnp.stack([(me - separation) % length, number])
        values = shift(run(where, [shift(sink, separation)])[0], -separation)
        total = values if total is None else total + values
    return total


def relayed(run, sink):
    me = lax.axis_index("tm")
    length = lax.axis_size("tm")
    planes = lax.axis_size("op")
    core, pair = me % 2, me // 2

    def exchange(values, moves):
        pairs = [
            (t * planes + z, u * planes + w)
            for t in range(length)
            for z in range(planes)
            for u, w in [moves(t, z)]
            if u is not None
        ]
        return lax.ppermute(values, ("tm", "op"), pairs)

    near = lambda t, z: (t + z) % 2 == 0
    partner = exchange(sink, lambda t, z: (t ^ 1, z))
    first = exchange(sink, lambda t, z: (t ^ 2, z) if near(t, z) else (t ^ 4, z))
    across = exchange(first, lambda t, z: (t ^ 4, z) if near(t, z) else (t ^ 2, z))
    other = exchange(first, lambda t, z: (t, z ^ 1) if near(t, z) else (None, None))
    beside = jnp.where(near(me, lax.axis_index("op")), first, other)
    lends_beside = (pair + core) % 2 == 0
    lent = exchange(jnp.where(lends_beside, beside, across), lambda t, z: (t ^ 1, z))

    even = pair % 2 == 0
    up, down = (me + 2) % length, (me - 2) % length
    where_partner = jnp.stack([me ^ 1, 1 + core])
    where_direct = jnp.stack([me ^ 2, jnp.where(even, 0, 3), me ^ 6, jnp.where(even, 3, 0)])
    where_lent = jnp.stack([jnp.where(core == 0, me - 1, me + 1) % length, 2 - core])

    values_partner = exchange(run(where_partner, [partner])[0], lambda t, z: (t ^ 1, z))
    values = run(where_direct, [beside, across])
    values_beside = exchange(values[0], lambda t, z: (t ^ 2, z))
    values_across = exchange(values[1], lambda t, z: (t ^ 6, z))
    values_lent = exchange(
        run(where_lent, [lent])[0], lambda t, z: ((t + 1 if t % 2 else t - 1) % length, z)
    )
    return values_partner + values_beside + values_across + values_lent


def shards(sources, sink, phase, task_table):
    table = lax.all_gather(task_table[:, 0], "tm")
    cosine = jnp.cos(phase)[:, None, :]
    sine = jnp.sin(phase)[:, None, :]

    def run(where, sinks):
        return contract(where.astype(jnp.int32), table, sources[0], cosine, sine, sinks)

    pairs = lax.axis_size("tm") // 2
    method = relayed if pairs == 4 and lax.axis_size("op") % 2 == 0 else direct
    return method(run, sink[0])[None]


def solution(mesh):
    return jax.shard_map(
        shards,
        mesh=mesh,
        in_specs=(
            P(("grp", "tm"), "op", None, None, None),
            P(("grp", "tm"), None, None, None),
            P(),
            P(None, ("grp", "tm"), "op"),
        ),
        out_specs=P(("grp", "tm"), "op", None, None),
        check_vma=False,
    )
```
